32 devices in a mesh: row: 4 (over y, x), col: 8 (over z, core).
Axes of the slice: x: 2, y: 2, z: 4, core: 2. Of those that a mesh axis runs over, the one named last changes fastest.
Arguments:
- wrapped: float32 [1, 4096, 8192], P(None, 'row', 'col'), may hold values from -2.8 to 2.8
- col_steps: int32 [1, 4, 8], P(None, 'row', 'col'), may hold values from -2 to 2, as said below
- row_steps: int32 [1, 4, 8], P(None, 'row', 'col'), may hold values from -2 to 2, as said below
Outputs:
- unwrapped: float32 [1, 4096, 8192], P(None, 'row', 'col')
The draws below stay inside these ranges and needn't reach their ends.
Inputs may be any that keep to these rules, and one draw needn't show every extreme that they name: `col_steps`: nonzero whole numbers; the last tile column has no edge. `row_steps`: nonzero whole numbers; the last tile row has no edge.
All inputs are finite; a program needn't handle non-finite values.
Results may differ from the reference program's by a relative error of at most 0.0003.
Values sent between devices are 32-bit elements; how exact they have to be, the bound alone decides.
No kernel may reach another device: no remote copies, remote signals or barrier semaphores. Data moves between devices by JAX's collectives and lax.ppermute only.
A program may use at most 64 MiB of HBM per device.

```python
import math
import jax
import jax.numpy as jnp
from jax import lax

FRAMES = 1
TILE_ROWS = 1024
TILE_COLS = 1024
ITERS = 2
IMAGE_ROWS = 4096
IMAGE_COLS = 8192
N_ROW = 4
N_COL = 8


TWO_PI = 2.0 * math.pi


def draw_wrapped(key, part):
    extent = (FRAMES, IMAGE_ROWS, IMAGE_COLS)
    levels = jax.random.randint(jax.random.fold_in(key, 1), extent, -3, 4)
    speckle = jax.random.randint(jax.random.fold_in(key, 2), extent, 0, 5)
    levels = jnp.where(speckle == 0, levels, 0)
    jitter = jnp.clip(0.04 * jax.random.normal(jax.random.fold_in(key, 3), extent, jnp.float32), -0.1, 0.1)
    return (TWO_PI / 7.0 * levels.astype(jnp.float32) + jitter).astype(jnp.float32)


def signed_steps(key):
    extent = (FRAMES, N_ROW, N_COL)
    magnitude = jax.random.randint(jax.random.fold_in(key, 1), extent, 1, 3)
    polarity = 2 * jax.random.randint(jax.random.fold_in(key, 2), extent, 0, 2) - 1
    return (magnitude * polarity).astype(jnp.int32)


def draw_col_steps(key, part):
    return signed_steps(jax.random.fold_in(key, 11))


def draw_row_steps(key, part):
    return signed_steps(jax.random.fold_in(key, 12))


def setup_inputs(seed: int = 0) -> dict:
    arg_keys = jax.random.split(jax.random.key(seed), 4)
    return {
        "wrapped": draw_wrapped(jax.random.fold_in(arg_keys[3], 71), 0),
        "col_steps": draw_col_steps(jax.random.fold_in(arg_keys[3], 71), 0),
        "row_steps": draw_row_steps(jax.random.fold_in(arg_keys[3], 71), 0),
    }


TWO_PI = 2.0 * math.pi


def wrap_diff(change):
    return change - TWO_PI * jnp.floor(change / TWO_PI + 0.5)


def unwrap_frame(inputs):
    wrapped, col_steps, row_steps = inputs
    grid_x = wrap_diff(wrapped[:, 1:] - wrapped[:, :-1])
    grid_x = jnp.concatenate([grid_x, jnp.zeros((IMAGE_ROWS, 1), grid_x.dtype)], axis=1)
    grid_y = wrap_diff(wrapped[1:, :] - wrapped[:-1, :])
    grid_y = jnp.concatenate([grid_y, jnp.zeros((1, IMAGE_COLS), grid_y.dtype)], axis=0)
    charge = (grid_x[:-1, :-1] + grid_y[:-1, 1:] - grid_x[1:, :-1] - grid_y[:-1, :-1]) / TWO_PI
    charge = jnp.pad(charge, ((1, 0), (1, 0)))
    weight = 1.0 / (1.0 + jnp.abs(charge))
    tiled_shape = (N_ROW, TILE_ROWS, N_COL, TILE_COLS)
    step_x = grid_x.reshape(tiled_shape)
    step_y = grid_y.reshape(tiled_shape)
    weight_tiles = weight.reshape(tiled_shape)
    along_cols = jnp.cumsum(step_x, axis=3) - step_x
    first_column = step_y[:, :, :, 0]
    downward = jnp.cumsum(first_column, axis=1) - first_column
    anchor = wrapped.reshape(tiled_shape)[:, 0, :, 0]
    current = (anchor[:, None, :] + downward)[:, :, :, None] + along_cols
    col_weight = weight_tiles[:, :, :, -1]
    cross_x = step_x[:, :, :, -1]
    row_weight = weight_tiles[:, -1, :, :]
    cross_y = step_y[:, -1, :, :]
    cycles_across = TWO_PI * col_steps.astype(jnp.float32)
    cycles_down = TWO_PI * row_steps.astype(jnp.float32)
    for sweep in range(ITERS):
        beyond_x = jnp.concatenate([current[:, :, 1:, 0], jnp.zeros((N_ROW, TILE_ROWS, 1), current.dtype)], axis=2)
        horizontal = jnp.sum(col_weight * (current[:, :, :, -1] + cross_x - beyond_x), axis=1) / jnp.sum(col_weight, axis=1)
        beyond_y = jnp.concatenate([current[1:, 0, :, :], jnp.zeros((1, N_COL, TILE_COLS), current.dtype)], axis=0)
        vertical = jnp.sum(row_weight * (current[:, -1, :, :] + cross_y - beyond_y), axis=2) / jnp.sum(row_weight, axis=2)
        horizontal = horizontal + cycles_across
        vertical = vertical + cycles_down
        prefix_across = jnp.cumsum(horizontal, axis=1) - horizontal
        prefix_down = jnp.cumsum(vertical, axis=0) - vertical
        offset = 0.5 * (prefix_across + prefix_across[0:1, :] + prefix_down + prefix_down[:, 0:1])
        current = current + offset[:, None, :, None]
    return (current / TWO_PI).reshape(IMAGE_ROWS, IMAGE_COLS)


def reference(wrapped, col_steps, row_steps):
    return lax.map(unwrap_frame, (wrapped, col_steps, row_steps))
```

```python
import functools
import math

import jax
import jax.numpy as jnp
from jax import lax
from jax.experimental import pallas as pl
from jax.experimental.pallas import tpu as pltpu
from jax.sharding import PartitionSpec as P

ITERS = 2
TWO_PI = 2.0 * math.pi
CYCLE = 1.0 / TWO_PI
LANES = 128


def iota(shape, dim):
    return lax.broadcasted_iota(jnp.int32, shape, dim)


def wraps(change):
    return jnp.floor(change + 0.5)


def along(line):
    return jnp.where(iota(line.shape, 1) == 0, 0.0, wraps(line - pltpu.roll(line, 1, 1)))


def upper_ones(length, width):
    shape = (length, width)
    return (iota(shape, 0) - (length - width) <= iota(shape, 1)).astype(jnp.bfloat16)


def prefix_blocks(counts, ones, width):
    length = counts.shape[1]
    narrow = counts.astype(jnp.bfloat16)
    return [
        jnp.dot(narrow[:, :stop], ones[length - stop :, :], preferred_element_type=jnp.float32)
        for stop in range(width, length + 1, width)
    ]


def integrate_kernel(w_ref, u_ref, cols_ref, rows_ref, ones, lower, last_phase, last_wraps, *, width):
    height, length = w_ref.shape
    step = pl.program_id(0)
    phase = w_ref[...] * CYCLE
    edge = phase[:, :LANES]

    @pl.when(step == 0)
    def _():
        ones[...] = upper_ones(length, width)
        lower[...] = (iota((height, height), 0) >= iota((height, height), 1)).astype(jnp.bfloat16)
        last_phase[...] = edge[0:1, :]
        last_wraps[...] = jnp.zeros_like(last_wraps)

    before = jnp.where(iota(edge.shape, 0) == 0, last_phase[...], pltpu.roll(edge, 1, 0))
    down = wraps(edge - before).astype(jnp.bfloat16)
    down = jnp.dot(lower[...], down, preferred_element_type=jnp.float32) + last_wraps[...]
    last_phase[...] = edge[height - 1 :, :]
    last_wraps[...] = down[height - 1 :, :]
    first = down[:, 0:1]
    blocks = prefix_blocks(along(phase), ones, width)
    for n, block in enumerate(blocks):
        span = slice(n * width, (n + 1) * width)
        total = first + block
        u_ref[:, span] = phase[:, span] - total
        rows_ref[0:1, span] = total[height - 1 :, :]
    rows_ref[1:3, :] = phase[height - 2 :, :]
    cols_ref[0:1, :] = total[:, width - LANES :].T[LANES - 1 :, :]
    cols_ref[1:3, :] = phase[:, length - LANES :].T[LANES - 2 :, :]


def side_sums(lines, halo, at_end, width):
    total, inner, outer = lines[0:1, :], lines[1:2, :], lines[2:3, :]
    lane = iota(total.shape, 1)
    length = total.shape[1]
    outer_wraps, halo_wraps = along(outer), along(halo)
    cross = wraps(outer - inner)
    charge = along(inner) + cross - outer_wraps - pltpu.roll(cross, 1, 1)
    weight = jnp.where(lane == 0, 0.0, 1.0 / (1.0 + jnp.abs(charge)))
    beyond = wraps(halo - outer)
    next_charge = outer_wraps + beyond - halo_wraps - pltpu.roll(beyond, 1, 1)
    next_weight = 1.0 / (1.0 + jnp.abs(next_charge))
    ones = upper_ones(length, width)
    halo_total = jnp.concatenate(
        [b[0:1, :] for b in prefix_blocks(jnp.broadcast_to(halo_wraps, (8, length)), ones, width)],
        axis=1,
    )
    jump = jnp.where(at_end, outer - total, halo_total - total - beyond)

    def add(values):
        return jnp.sum(values, axis=1, keepdims=True)

    return [
        add(weight * jump),
        add(weight),
        add(jnp.where(lane == 0, jump, 0.0)),
        add(jnp.where(lane == length - 1, next_weight, 0.0)),
    ]


def edges_kernel(
    right_steps, down_steps, cols_ref, rows_ref, right_ref, below_ref, table_ref, *, grid, widths
):
    row, col = lax.axis_index("row"), lax.axis_index("col")
    values = side_sums(cols_ref[...], right_ref[...] * CYCLE, col == grid[1] - 1, widths[0])
    values += side_sums(rows_ref[...], below_ref[...] * CYCLE, row == grid[0] - 1, widths[1])
    shape = table_ref.shape
    values += [
        jnp.full((1, 1), right_steps[0].astype(jnp.float32)),
        jnp.full((1, 1), down_steps[0].astype(jnp.float32)),
    ]
    table = jnp.zeros(shape, jnp.float32)
    for n, value in enumerate(values):
        table = jnp.where(iota(shape, 0) == n, value, table)
    table_ref[...] = jnp.where(iota(shape, 1) == row * grid[1] + col, table, 0.0)


def tile_offsets(table, grid):
    tile_rows, tile_cols = grid
    shape = (8, table.shape[1])
    size = table.shape[1]
    lane = iota(shape, 1)
    r, c = lane // tile_cols, lane % tile_cols
    there = lane < tile_rows * tile_cols

    def line(n):
        return jnp.broadcast_to(table[n : n + 1, :], shape)

    first = jnp.where(r == 0, 1.0, pltpu.roll(line(7), tile_cols, 1))
    across = (line(0) + first * line(2)) / (line(1) + first) + line(8)
    across = jnp.where(there, across, 0.0)
    first = jnp.where(c == 0, 1.0, pltpu.roll(line(3), 1, 1))
    down = (line(4) + first * line(6)) / (line(5) + first) + line(9)
    down = jnp.where(there, down, 0.0)
    source, target = iota((size, size), 0), iota((size, size), 1)
    sr, sc = source // tile_cols, source % tile_cols
    tr, tc = target // tile_cols, target % tile_cols
    use_across = jnp.where(sc < tc, 0.5, 0.0)
    use_across = jnp.where(sr == tr, use_across, 0.0) + jnp.where(sr == 0, use_across, 0.0)
    use_down = jnp.where(sr < tr, 0.5, 0.0)
    use_down = jnp.where(sc == tc, use_down, 0.0) + jnp.where(sc == 0, use_down, 0.0)
    dot = functools.partial(
        jnp.dot, precision=lax.Precision.HIGHEST, preferred_element_type=jnp.float32
    )
    totals = jnp.zeros(shape, jnp.float32)
    for _ in range(ITERS):
        right = jnp.where(c == tile_cols - 1, 0.0, pltpu.roll(totals, size - 1, 1))
        below = jnp.where(r == tile_rows - 1, 0.0, pltpu.roll(totals, size - tile_cols, 1))
        horizontal = across + totals - right
        vertical = down + totals - below
        step = dot(horizontal, use_across) + dot(vertical, use_down)
        totals = totals + jnp.where(there, step, 0.0)
    return totals


def shift_kernel(table_ref, u_ref, out_ref, offset, *, grid):
    @pl.when(pl.program_id(0) == 0)
    def _():
        totals = tile_offsets(table_ref[...], grid)[0:1, :]
        me = lax.axis_index("row") * grid[1] + lax.axis_index("col")
        mine = jnp.sum(jnp.where(iota(totals.shape, 1) == me, totals, 0.0), axis=1, keepdims=True)
        offset[...] = jnp.broadcast_to(mine, offset.shape)

    out_ref[...] = u_ref[...] + offset[0:1, 0:1]


def integrate(tile):
    rows, cols = tile.shape
    height, width = math.gcd(rows, 256), math.gcd(cols, 256)
    return pl.pallas_call(
        functools.partial(integrate_kernel, width=width),
        grid=(rows // height,),
        in_specs=[pl.BlockSpec((height, cols), lambda i: (i, 0))],
        out_specs=[
            pl.BlockSpec((height, cols), lambda i: (i, 0)),
            pl.BlockSpec((8, height), lambda i: (0, i)),
            pl.BlockSpec((8, cols), lambda i: (0, 0)),
        ],
        out_shape=[
            jax.ShapeDtypeStruct((rows, cols), jnp.float32),
            jax.ShapeDtypeStruct((8, rows), jnp.float32),
            jax.ShapeDtypeStruct((8, cols), jnp.float32),
        ],
        scratch_shapes=[
            pltpu.VMEM((cols, width), jnp.bfloat16),
            pltpu.VMEM((height, height), jnp.bfloat16),
            pltpu.VMEM((1, LANES), jnp.float32),
            pltpu.VMEM((1, LANES), jnp.float32),
        ],
        name="integrate",
    )(tile)


def gathered(table, grid):
    for axis, count in zip(("col", "row"), grid[::-1]):
        if count & (count - 1):
            table = lax.psum(table, axis)
            continue
        bit = 1
        while bit < count:
            table = table + lax.ppermute(table, axis, [(i, i ^ bit) for i in range(count)])
            bit *= 2
    return table


def on_device(grid, wrapped, col_steps, row_steps):
    frames, rows, cols = wrapped.shape
    widths = (math.gcd(rows, 256), math.gcd(cols, 256))
    slots = -(-grid[0] * grid[1] // LANES) * LANES
    smem = pl.BlockSpec(memory_space=pltpu.SMEM)
    vmem = pl.BlockSpec(memory_space=pltpu.VMEM)
    outs = []
    for f in range(frames):
        tile = wrapped[f]
        right = lax.ppermute(tile[:, 0][None, :], "col", [(i + 1, i) for i in range(grid[1] - 1)])
        below = lax.ppermute(tile[0:1, :], "row", [(i + 1, i) for i in range(grid[0] - 1)])
        cycles, col_lines, row_lines = integrate(tile)
        table = pl.pallas_call(
            functools.partial(edges_kernel, grid=grid, widths=widths),
            in_specs=[smem, smem, vmem, vmem, vmem, vmem],
            out_specs=vmem,
            out_shape=jax.ShapeDtypeStruct((16, slots), jnp.float32),
            name="edges",
        )(col_steps[f, 0], row_steps[f, 0], col_lines, row_lines, right, below)
        table = gathered(table, grid)
        height = math.gcd(rows, 256)
        outs.append(
            pl.pallas_call(
                functools.partial(shift_kernel, grid=grid),
                grid=(rows // height,),
                in_specs=[
                    pl.BlockSpec((16, slots), lambda i: (0, 0)),
                    pl.BlockSpec((height, cols), lambda i: (i, 0)),
                ],
                out_specs=pl.BlockSpec((height, cols), lambda i: (i, 0)),
                out_shape=jax.ShapeDtypeStruct((rows, cols), jnp.float32),
                scratch_shapes=[pltpu.VMEM((8, LANES), jnp.float32)],
                name="shift",
            )(table, cycles)
        )
    return jnp.stack(outs)


def solution(mesh):
    grid = (mesh.shape["row"], mesh.shape["col"])
    spec = P(None, "row", "col")
    return jax.shard_map(
        functools.partial(on_device, grid),
        mesh=mesh,
        in_specs=(spec, spec, spec),
        out_specs=spec,
        check_vma=False,
    )
```

```python
import functools
import math

import jax
import jax.numpy as jnp
from jax import lax
from jax.experimental import pallas as pl
from jax.experimental.pallas import tpu as pltpu
from jax.sharding import PartitionSpec as P

ITERS = 2
TWO_PI = 2.0 * math.pi
CYCLE = 1.0 / TWO_PI
LANES = 128
VMEM_LIMIT = 32 * 2**20


def iota(shape, dim):
    return lax.broadcasted_iota(jnp.int32, shape, dim)


def wraps(change):
    return jnp.floor(change + 0.5)


def along(line):
    return jnp.where(iota(line.shape, 1) == 0, 0.0, wraps(line - pltpu.roll(line, 1, 1)))


def upper_ones(length, width):
    shape = (length, width)
    return (iota(shape, 0) - (length - width) <= iota(shape, 1)).astype(jnp.bfloat16)


def prefix_blocks(counts, ones, width):
    length = counts.shape[1]
    narrow = counts.astype(jnp.bfloat16)
    return [
        jnp.dot(narrow[:, :stop], ones[length - stop :, :], preferred_element_type=jnp.float32)
        for stop in range(width, length + 1, width)
    ]


def integrate_kernel(w_ref, u_ref, cols_ref, rows_ref, tile, sems, *, height, width):
    rows, length = tile.shape
    copies = []
    for step in range(rows // height):
        part = pl.ds(step * height, height)
        copies.append(pltpu.make_async_copy(w_ref.at[part], tile.at[part], sems.at[step]))
        copies[-1].start()
    ones = upper_ones(length, width)
    lower = (iota((height, height), 0) >= iota((height, height), 1)).astype(jnp.bfloat16)
    last_wraps = jnp.zeros((1, LANES), jnp.float32)
    last_phase = None
    for step, copy in enumerate(copies):
        copy.wait()
        part = slice(step * height, (step + 1) * height)
        phase = tile[part, :] * CYCLE
        edge = phase[:, :LANES]
        if last_phase is None:
            last_phase = edge[0:1, :]
        before = jnp.where(iota(edge.shape, 0) == 0, last_phase, pltpu.roll(edge, 1, 0))
        down = wraps(edge - before).astype(jnp.bfloat16)
        down = jnp.dot(lower, down, preferred_element_type=jnp.float32) + last_wraps
        last_phase, last_wraps = edge[height - 1 :, :], down[height - 1 :, :]
        first = down[:, 0:1]
        blocks = prefix_blocks(along(phase), ones, width)
        for n, block in enumerate(blocks):
            span = slice(n * width, (n + 1) * width)
            total = first + block
            u_ref[part, span] = phase[:, span] - total
            if step == len(copies) - 1:
                rows_ref[0:1, span] = total[height - 1 :, :]
        cols_ref[0:1, part] = total[:, width - LANES :].T[LANES - 1 :, :]
        cols_ref[1:3, part] = phase[:, length - LANES :].T[LANES - 2 :, :]
    rows_ref[1:3, :] = phase[height - 2 :, :]


def side_sums(lines, halo, cycles, at_end, width):
    total, inner, outer = lines[0:1, :], lines[1:2, :], lines[2:3, :]
    lane = iota(total.shape, 1)
    length = total.shape[1]
    outer_wraps, halo_wraps = along(outer), along(halo)
    cross = wraps(outer - inner)
    charge = along(inner) + cross - outer_wraps - pltpu.roll(cross, 1, 1)
    weight = jnp.where(lane == 0, 0.0, 1.0 / (1.0 + jnp.abs(charge)))
    beyond = wraps(halo - outer)
    next_charge = outer_wraps + beyond - halo_wraps - pltpu.roll(beyond, 1, 1)
    next_weight = 1.0 / (1.0 + jnp.abs(next_charge))
    ones = upper_ones(length, width)
    halo_total = jnp.concatenate(
        [b[0:1, :] for b in prefix_blocks(jnp.broadcast_to(halo_wraps, (8, length)), ones, width)],
        axis=1,
    )
    jump = jnp.where(at_end, outer - total, halo_total - total - beyond) + cycles

    def add(values):
        return jnp.sum(values, axis=1, keepdims=True)

    return [
        add(weight * jump),
        add(weight),
        add(jnp.where(lane == 0, jump, 0.0)),
        add(jnp.where(lane == length - 1, next_weight, 0.0)),
    ]


def edges_kernel(
    right_steps, down_steps, cols_ref, rows_ref, right_ref, below_ref, table_ref, *, grid, widths
):
    row, col = lax.axis_index("row"), lax.axis_index("col")
    values = side_sums(cols_ref[...], right_ref[...] * CYCLE, right_steps[0, 0, 0].astype(jnp.float32), col == grid[1] - 1, widths[0])
    values += side_sums(rows_ref[...], below_ref[...] * CYCLE, down_steps[0, 0, 0].astype(jnp.float32), row == grid[0] - 1, widths[1])
    shape = table_ref.shape
    table = jnp.zeros(shape, jnp.float32)
    for n, value in enumerate(values):
        table = jnp.where(iota(shape, 0) == n, value, table)
    table_ref[...] = jnp.where(iota(shape, 1) == row * grid[1] + col, table, 0.0)


def tile_offsets(table, grid):
    tile_rows, tile_cols = grid
    shape = (8, table.shape[1])
    size = table.shape[1]
    lane = iota(shape, 1)
    r, c = lane // tile_cols, lane % tile_cols
    there = lane < tile_rows * tile_cols

    def line(n):
        return jnp.broadcast_to(table[n : n + 1, :], shape)

    first = jnp.where(r == 0, 1.0, pltpu.roll(line(7), tile_cols, 1))
    across = (line(0) + first * line(2)) / (line(1) + first)
    across = jnp.where(there, across, 0.0)
    first = jnp.where(c == 0, 1.0, pltpu.roll(line(3), 1, 1))
    down = (line(4) + first * line(6)) / (line(5) + first)
    down = jnp.where(there, down, 0.0)
    source, target = iota((size, size), 0), iota((size, size), 1)
    sr, sc = source // tile_cols, source % tile_cols
    tr, tc = target // tile_cols, target % tile_cols
    use_across = jnp.where(sc < tc, 0.5, 0.0)
    use_across = jnp.where(sr == tr, use_across, 0.0) + jnp.where(sr == 0, use_across, 0.0)
    use_down = jnp.where(sr < tr, 0.5, 0.0)
    use_down = jnp.where(sc == tc, use_down, 0.0) + jnp.where(sc == 0, use_down, 0.0)
    dot = functools.partial(
        jnp.dot, precision=lax.Precision.HIGHEST, preferred_element_type=jnp.float32
    )
    totals = jnp.zeros(shape, jnp.float32)
    for _ in range(ITERS):
        right = jnp.where(c == tile_cols - 1, 0.0, pltpu.roll(totals, size - 1, 1))
        below = jnp.where(r == tile_rows - 1, 0.0, pltpu.roll(totals, size - tile_cols, 1))
        horizontal = across + totals - right
        vertical = down + totals - below
        step = dot(horizontal, use_across) + dot(vertical, use_down)
        totals = totals + jnp.where(there, step, 0.0)
    return totals


def shift_kernel(mine_ref, theirs_ref, u_ref, out_ref, moved, sems, *, grid, height):
    totals = tile_offsets(mine_ref[...] + theirs_ref[...], grid)[0:1, :]
    me = lax.axis_index("row") * grid[1] + lax.axis_index("col")
    offset = jnp.sum(jnp.where(iota(totals.shape, 1) == me, totals, 0.0), axis=1, keepdims=True)
    copies = []
    for step in range(u_ref.shape[0] // height):
        part = pl.ds(step * height, height)
        moved[part, :] = u_ref[part, :] + offset
        copies.append(pltpu.make_async_copy(moved.at[part], out_ref.at[part], sems.at[step]))
        copies[-1].start()
    for copy in copies:
        copy.wait()


def integrate(tile):
    rows, cols = tile.shape
    height, width = math.gcd(rows, 256), math.gcd(cols, 256)
    vmem = pl.BlockSpec(memory_space=pltpu.VMEM)
    return pl.pallas_call(
        functools.partial(integrate_kernel, height=height, width=width),
        in_specs=[pl.BlockSpec(memory_space=pltpu.HBM)],
        out_specs=[vmem, vmem, vmem],
        out_shape=[
            pltpu.VMEM((rows, cols), jnp.float32),
            pltpu.VMEM((8, rows), jnp.float32),
            pltpu.VMEM((8, cols), jnp.float32),
        ],
        scratch_shapes=[
            pltpu.VMEM((rows, cols), jnp.float32),
            pltpu.SemaphoreType.DMA((rows // height,)),
        ],
        compiler_params=pltpu.CompilerParams(vmem_limit_bytes=VMEM_LIMIT),
            name="integrate",
    )(pltpu.with_memory_space_constraint(tile, pltpu.HBM))


def near(array):
    return pltpu.with_memory_space_constraint(array, pltpu.VMEM)


def gathered(table, grid):
    theirs = jnp.zeros_like(table)
    for axis, count in zip(("col", "row"), grid[::-1]):
        if count & (count - 1):
            table, theirs = lax.psum(table + theirs, axis), jnp.zeros_like(table)
            continue
        bit = 1
        while bit < count:
            table = table + theirs
            theirs = lax.ppermute(table, axis, [(i, i ^ bit) for i in range(count)])
            bit *= 2
    return near(table), near(theirs)


def on_device(grid, wrapped, col_steps, row_steps):
    frames, rows, cols = wrapped.shape
    widths = (math.gcd(rows, 256), math.gcd(cols, 256))
    slots = -(-grid[0] * grid[1] // LANES) * LANES
    smem = pl.BlockSpec(memory_space=pltpu.SMEM)
    vmem = pl.BlockSpec(memory_space=pltpu.VMEM)
    outs = []
    for f in range(frames):
        tile = wrapped[f]
        right = lax.ppermute(tile[:, 0][None, :], "col", [(i + 1, i) for i in range(grid[1] - 1)])
        below = lax.ppermute(tile[0:1, :], "row", [(i + 1, i) for i in range(grid[0] - 1)])
        cycles, col_lines, row_lines = integrate(tile)
        table = pl.pallas_call(
            functools.partial(edges_kernel, grid=grid, widths=widths),
            in_specs=[smem, smem, vmem, vmem, vmem, vmem],
            out_specs=vmem,
            out_shape=pltpu.VMEM((8, slots), jnp.float32),
            compiler_params=pltpu.CompilerParams(vmem_limit_bytes=VMEM_LIMIT),
            name="edges",
        )(
            col_steps[f : f + 1], row_steps[f : f + 1], near(col_lines), near(row_lines), near(right), near(below)
        )
        mine, theirs = gathered(table, grid)
        height = math.gcd(rows, 128)
        outs.append(
            pl.pallas_call(
                functools.partial(shift_kernel, grid=grid, height=height),
                in_specs=[vmem, vmem, vmem],
                out_specs=pl.BlockSpec(memory_space=pl.ANY),
                out_shape=jax.ShapeDtypeStruct((rows, cols), jnp.float32),
                scratch_shapes=[
                    pltpu.VMEM((rows, cols), jnp.float32),
                    pltpu.SemaphoreType.DMA((rows // height,)),
                ],
                compiler_params=pltpu.CompilerParams(vmem_limit_bytes=VMEM_LIMIT),
            name="shift",
            )(mine, theirs, near(cycles))
        )
    return jnp.stack(outs)


def solution(mesh):
    grid = (mesh.shape["row"], mesh.shape["col"])
    spec = P(None, "row", "col")
    return jax.shard_map(
        functools.partial(on_device, grid),
        mesh=mesh,
        in_specs=(spec, spec, spec),
        out_specs=spec,
        check_vma=False,
    )
```

```python
import functools
import math

import jax
import jax.numpy as jnp
from jax import lax
from jax.experimental import pallas as pl
from jax.experimental.pallas import tpu as pltpu
from jax.sharding import PartitionSpec as P

ITERS = 2
TWO_PI = 2.0 * math.pi
CYCLE = 1.0 / TWO_PI
LANES = 128
VMEM_LIMIT = 32 * 2**20


def iota(shape, dim):
    return lax.broadcasted_iota(jnp.int32, shape, dim)


def wraps(change):
    return jnp.floor(change + 0.5)


def along(line):
    return jnp.where(iota(line.shape, 1) == 0, 0.0, wraps(line - pltpu.roll(line, 1, 1)))


def upper_ones(length, width):
    shape = (length, width)
    return (iota(shape, 0) - (length - width) <= iota(shape, 1)).astype(jnp.bfloat16)


def prefix_blocks(counts, ones, width):
    length = counts.shape[1]
    narrow = counts.astype(jnp.bfloat16)
    return [
        jnp.dot(narrow[:, :stop], ones[length - stop :, :], preferred_element_type=jnp.float32)
        for stop in range(width, length + 1, width)
    ]


def integrate_kernel(w_ref, u_ref, cols_ref, rows_ref, tile, sems, *, height, width):
    rows, length = tile.shape
    copies = []
    for step in range(rows // height):
        part = pl.ds(step * height, height)
        copies.append(pltpu.make_async_copy(w_ref.at[part], tile.at[part], sems.at[step]))
        copies[-1].start()
    ones = upper_ones(length, width)
    lower = (iota((height, height), 0) >= iota((height, height), 1)).astype(jnp.bfloat16)
    last_wraps = jnp.zeros((1, LANES), jnp.float32)
    last_phase = None
    for step, copy in enumerate(copies):
        copy.wait()
        part = slice(step * height, (step + 1) * height)
        phase = tile[part, :] * CYCLE
        edge = phase[:, :LANES]
        if last_phase is None:
            last_phase = edge[0:1, :]
        before = jnp.where(iota(edge.shape, 0) == 0, last_phase, pltpu.roll(edge, 1, 0))
        down = wraps(edge - before).astype(jnp.bfloat16)
        down = jnp.dot(lower, down, preferred_element_type=jnp.float32) + last_wraps
        last_phase, last_wraps = edge[height - 1 :, :], down[height - 1 :, :]
        first = down[:, 0:1]
        blocks = prefix_blocks(along(phase), ones, width)
        for n, block in enumerate(blocks):
            span = slice(n * width, (n + 1) * width)
            total = first + block
            u_ref[part, span] = phase[:, span] - total
            if step == len(copies) - 1:
                rows_ref[0:1, span] = total[height - 1 :, :]
        cols_ref[0:1, part] = total[:, width - LANES :].T[LANES - 1 :, :]
        cols_ref[1:3, part] = phase[:, length - LANES :].T[LANES - 2 :, :]
    rows_ref[1:3, :] = phase[height - 2 :, :]


def side_sums(lines, halo, cycles, at_end, width):
    total, inner, outer = lines[0:1, :], lines[1:2, :], lines[2:3, :]
    lane = iota(total.shape, 1)
    length = total.shape[1]
    outer_wraps, halo_wraps = along(outer), along(halo)
    cross = wraps(outer - inner)
    charge = along(inner) + cross - outer_wraps - pltpu.roll(cross, 1, 1)
    weight = jnp.where(lane == 0, 0.0, 1.0 / (1.0 + jnp.abs(charge)))
    beyond = wraps(halo - outer)
    next_charge = outer_wraps + beyond - halo_wraps - pltpu.roll(beyond, 1, 1)
    next_weight = 1.0 / (1.0 + jnp.abs(next_charge))
    ones = upper_ones(length, width)
    halo_total = jnp.concatenate(
        [b[0:1, :] for b in prefix_blocks(jnp.broadcast_to(halo_wraps, (8, length)), ones, width)],
        axis=1,
    )
    jump = jnp.where(at_end, outer - total, halo_total - total - beyond) + cycles

    def add(values):
        return jnp.sum(values, axis=1, keepdims=True)

    return [
        add(weight * jump),
        add(weight),
        add(jnp.where(lane == 0, jump, 0.0)),
        add(jnp.where(lane == length - 1, next_weight, 0.0)),
    ]


def edges_kernel(
    right_steps, down_steps, cols_ref, rows_ref, right_ref, below_ref, table_ref, *, grid, widths
):
    row, col = lax.axis_index("row"), lax.axis_index("col")
    values = side_sums(cols_ref[...], right_ref[...] * CYCLE, right_steps[0, 0, 0].astype(jnp.float32), col == grid[1] - 1, widths[0])
    values += side_sums(rows_ref[...], below_ref[...] * CYCLE, down_steps[0, 0, 0].astype(jnp.float32), row == grid[0] - 1, widths[1])
    shape = table_ref.shape
    table = jnp.zeros(shape, jnp.float32)
    for n, value in enumerate(values):
        table = jnp.where(iota(shape, 0) == n, value, table)
    table_ref[...] = jnp.where(iota(shape, 1) == row * grid[1] + col, table, 0.0)


def tile_offsets(table, grid):
    tile_rows, tile_cols = grid
    shape = (8, table.shape[1])
    size = table.shape[1]
    lane = iota(shape, 1)
    r, c = lane // tile_cols, lane % tile_cols
    there = lane < tile_rows * tile_cols

    def line(n):
        return jnp.broadcast_to(table[n : n + 1, :], shape)

    first = jnp.where(r == 0, 1.0, pltpu.roll(line(7), tile_cols, 1))
    across = (line(0) + first * line(2)) / (line(1) + first)
    across = jnp.where(there, across, 0.0)
    first = jnp.where(c == 0, 1.0, pltpu.roll(line(3), 1, 1))
    down = (line(4) + first * line(6)) / (line(5) + first)
    down = jnp.where(there, down, 0.0)
    source, target = iota((size, size), 0), iota((size, size), 1)
    sr, sc = source // tile_cols, source % tile_cols
    tr, tc = target // tile_cols, target % tile_cols
    use_across = jnp.where(sc < tc, 0.5, 0.0)
    use_across = jnp.where(sr == tr, use_across, 0.0) + jnp.where(sr == 0, use_across, 0.0)
    use_down = jnp.where(sr < tr, 0.5, 0.0)
    use_down = jnp.where(sc == tc, use_down, 0.0) + jnp.where(sc == 0, use_down, 0.0)
    dot = functools.partial(
        jnp.dot, precision=lax.Precision.HIGHEST, preferred_element_type=jnp.float32
    )
    totals = jnp.zeros(shape, jnp.float32)
    for _ in range(ITERS):
        right = jnp.where(c == tile_cols - 1, 0.0, pltpu.roll(totals, size - 1, 1))
        below = jnp.where(r == tile_rows - 1, 0.0, pltpu.roll(totals, size - tile_cols, 1))
        horizontal = across + totals - right
        vertical = down + totals - below
        step = dot(horizontal, use_across) + dot(vertical, use_down)
        totals = totals + jnp.where(there, step, 0.0)
    return totals


def shift_kernel(mine_ref, theirs_ref, u_ref, out_ref, moved, sems, *, grid, height):
    totals = tile_offsets(mine_ref[...] + theirs_ref[...], grid)[0:1, :]
    me = lax.axis_index("row") * grid[1] + lax.axis_index("col")
    offset = jnp.sum(jnp.where(iota(totals.shape, 1) == me, totals, 0.0), axis=1, keepdims=True)
    copies = []
    for step in range(u_ref.shape[0] // height):
        part = pl.ds(step * height, height)
        moved[part, :] = u_ref[part, :] + offset
        copies.append(pltpu.make_async_copy(moved.at[part], out_ref.at[part], sems.at[step]))
        copies[-1].start()
    for copy in copies:
        copy.wait()


def integrate(tile):
    rows, cols = tile.shape
    height, width = math.gcd(rows, 512), math.gcd(cols, 256)
    vmem = pl.BlockSpec(memory_space=pltpu.VMEM)
    return pl.pallas_call(
        functools.partial(integrate_kernel, height=height, width=width),
        in_specs=[pl.BlockSpec(memory_space=pltpu.HBM)],
        out_specs=[vmem, vmem, vmem],
        out_shape=[
            pltpu.VMEM((rows, cols), jnp.float32),
            pltpu.VMEM((8, rows), jnp.float32),
            pltpu.VMEM((8, cols), jnp.float32),
        ],
        scratch_shapes=[
            pltpu.VMEM((rows, cols), jnp.float32),
            pltpu.SemaphoreType.DMA((rows // height,)),
        ],
        compiler_params=pltpu.CompilerParams(vmem_limit_bytes=VMEM_LIMIT),
            name="integrate",
    )(pltpu.with_memory_space_constraint(tile, pltpu.HBM))


def near(array):
    return pltpu.with_memory_space_constraint(array, pltpu.VMEM)


def gathered(table, grid):
    theirs = jnp.zeros_like(table)
    for axis, count in zip(("row", "col"), grid):
        if count & (count - 1):
            table, theirs = lax.psum(table + theirs, axis), jnp.zeros_like(table)
            continue
        bit = count // 2
        while bit:
            table = table + theirs
            theirs = lax.ppermute(table, axis, [(i, i ^ bit) for i in range(count)])
            bit //= 2
    return near(table), near(theirs)


def on_device(grid, wrapped, col_steps, row_steps):
    frames, rows, cols = wrapped.shape
    widths = (math.gcd(rows, 256), math.gcd(cols, 256))
    slots = -(-grid[0] * grid[1] // LANES) * LANES
    smem = pl.BlockSpec(memory_space=pltpu.SMEM)
    vmem = pl.BlockSpec(memory_space=pltpu.VMEM)
    outs = []
    for f in range(frames):
        tile = wrapped[f]
        right = lax.ppermute(tile[:, 0][None, :], "col", [(i + 1, i) for i in range(grid[1] - 1)])
        below = lax.ppermute(tile[0:1, :], "row", [(i + 1, i) for i in range(grid[0] - 1)])
        cycles, col_lines, row_lines = integrate(tile)
        table = pl.pallas_call(
            functools.partial(edges_kernel, grid=grid, widths=widths),
            in_specs=[smem, smem, vmem, vmem, vmem, vmem],
            out_specs=vmem,
            out_shape=pltpu.VMEM((8, slots), jnp.float32),
            compiler_params=pltpu.CompilerParams(vmem_limit_bytes=VMEM_LIMIT),
            name="edges",
        )(
            col_steps[f : f + 1], row_steps[f : f + 1], near(col_lines), near(row_lines), near(right), near(below)
        )
        mine, theirs = gathered(table, grid)
        height = math.gcd(rows, 128)
        outs.append(
            pl.pallas_call(
                functools.partial(shift_kernel, grid=grid, height=height),
                in_specs=[vmem, vmem, vmem],
                out_specs=pl.BlockSpec(memory_space=pl.ANY),
                out_shape=jax.ShapeDtypeStruct((rows, cols), jnp.float32),
                scratch_shapes=[
                    pltpu.VMEM((rows, cols), jnp.float32),
                    pltpu.SemaphoreType.DMA((rows // height,)),
                ],
                compiler_params=pltpu.CompilerParams(vmem_limit_bytes=VMEM_LIMIT),
            name="shift",
            )(mine, theirs, near(cycles))
        )
    return jnp.stack(outs)


def solution(mesh):
    grid = (mesh.shape["row"], mesh.shape["col"])
    spec = P(None, "row", "col")
    return jax.shard_map(
        functools.partial(on_device, grid),
        mesh=mesh,
        in_specs=(spec, spec, spec),
        out_specs=spec,
        check_vma=False,
    )
```
